8 devices in a mesh: dp: 1 (over z), row: 2 (over y), col: 4 (over x, core).
Axes of the slice: x: 2, y: 2, z: 1, core: 2. Of those that a mesh axis runs over, the one named last changes fastest.
Arguments:
- x: bfloat16 [1024, 1280], P(('dp', 'row', 'col'))
- route_idx: int32 [1024, 6], P(('dp', 'row', 'col'))
- gates: float32 [1024, 6], P(('dp', 'row', 'col'))
- w1: bfloat16 [160, 1280, 384], P(('row', 'col'))
- w3: bfloat16 [160, 1280, 384], P(('row', 'col'))
- w2: bfloat16 [160, 384, 1280], P(('row', 'col'))
- dy: bfloat16 [1024, 1280], P(('dp', 'row', 'col'))
Outputs:
- output 1: bfloat16 [1024, 1280], P(('dp', 'row', 'col'))
- output 2: bfloat16 [1024, 1280], P(('dp', 'row', 'col'))
- output 3: float32 [1024, 6], P(('dp', 'row', 'col'))
- output 4: float32 [160, 1280, 384], P(('dp', 'row', 'col'))
- output 5: float32 [160, 1280, 384], P(('dp', 'row', 'col'))
- output 6: float32 [160, 384, 1280], P(('dp', 'row', 'col'))
All inputs are finite; a program needn't handle non-finite values.
Results may differ from the reference program's by a relative error of at most 0.0078903.
Values are sent between devices in bfloat16 or wider.
A program may use at most 1 GiB of HBM per device.

```python
import jax
import jax.numpy as jnp
from jax import lax

TOK = 128
NDEV = 8
D = 1280
FF = 384
EXPERTS = 160
TOP = 6

TG = NDEV * TOK
CAP = (4 * TOK * TOP + EXPERTS - 1) // EXPERTS
CG = NDEV * CAP
NH = max(1, min(TOP // 2, (8 * TOP) // NDEV))
HOT = 2 * EXPERTS // NDEV
NCOLD = EXPERTS - HOT


def setup_inputs(seed: int = 0, part: int = 0) -> dict:
    kw = jax.random.split(jax.random.key(seed), 3)
    kp = jax.random.split(jax.random.fold_in(jax.random.key(seed + 1), part), 8)
    w1 = (jax.random.normal(kw[0], (EXPERTS, D, FF), jnp.float32) * D ** -0.5).astype(jnp.bfloat16)
    w3 = (jax.random.normal(kw[1], (EXPERTS, D, FF), jnp.float32) * D ** -0.5).astype(jnp.bfloat16)
    w2 = (jax.random.normal(kw[2], (EXPERTS, FF, D), jnp.float32) * FF ** -0.5).astype(jnp.bfloat16)
    dmax = min(NH, HOT - NH, TOP - NH)
    sh = jax.random.randint(kp[2], (), 0, HOT)
    sc = jax.random.randint(kp[3], (), 0, NCOLD)
    dd = jax.random.randint(kp[0], (NDEV, TOK // 2), 0, dmax + 1)
    nh = jnp.stack([NH + dd, NH - dd], axis=-1).reshape(NDEV, TOK)
    nc = TOP - nh
    sth = jnp.cumsum(nh, axis=1) - nh
    stc = jnp.cumsum(nc, axis=1) - nc
    dev = jnp.arange(NDEV)[:, None, None]
    j = jnp.arange(TOP)[None, None, :]
    hot_ids = (sh + dev * (TOK * NH) + sth[:, :, None] + j) % HOT
    cold_ids = HOT + (sc + dev * (TOK * (TOP - NH)) + stc[:, :, None] + j - nh[:, :, None]) % NCOLD
    ids = jnp.where(j < nh[:, :, None], hot_ids, cold_ids).reshape(TG, TOP)
    ids = jax.random.permutation(kp[4], ids, axis=1, independent=True).astype(jnp.int32)
    gu = jax.random.uniform(kp[5], (TG, TOP), jnp.float32, 0.5, 1.5)
    gates = gu / jnp.sum(gu, axis=1, keepdims=True)
    x = jax.random.normal(kp[6], (TG, D), jnp.float32).astype(jnp.bfloat16)
    dy = jax.random.normal(kp[7], (TG, D), jnp.float32).astype(jnp.bfloat16)
    return {'x': x, 'route_idx': ids, 'gates': gates, 'w1': w1, 'w3': w3, 'w2': w2, 'dy': dy}


def reference(x, route_idx, gates, w1, w3, w2, dy):
    n = TG * TOP
    ef = route_idx.reshape(n)
    order = jnp.argsort(ef, stable=True).astype(jnp.int32)
    es = ef[order]
    first = jnp.searchsorted(es, es, side='left').astype(jnp.int32)
    rank = jnp.arange(n, dtype=jnp.int32) - first
    tab = jnp.full((EXPERTS, CG), n, jnp.int32).at[es, rank].set(order)
    gf = gates.reshape(n)

    def body(carry, inp):
        y_acc, dx_acc, dg = carry
        te, a1, a3, a2 = inp
        valid = te < n
        ai = jnp.minimum(te, n - 1)
        tk = ai // TOP
        xr = x[tk]
        xs = jnp.where(valid[:, None], xr, jnp.zeros_like(xr))
        u = jnp.dot(xs, a1, preferred_element_type=jnp.float32).astype(jnp.bfloat16).astype(jnp.float32)
        v = jnp.dot(xs, a3, preferred_element_type=jnp.float32).astype(jnp.bfloat16).astype(jnp.float32)
        sg = jax.nn.sigmoid(u)
        a = (u * sg * v).astype(jnp.bfloat16)
        o = jnp.dot(a, a2, preferred_element_type=jnp.float32).astype(jnp.bfloat16).astype(jnp.float32)
        g = jnp.where(valid, gf[ai], 0.0)
        y_acc = y_acc.at[tk].add(g[:, None] * o)
        dys = dy[tk].astype(jnp.float32)
        dg = dg.at[ai].add(jnp.where(valid, jnp.sum(dys * o, axis=1), 0.0))
        do = (g[:, None] * dys).astype(jnp.bfloat16)
        gw2 = jnp.dot(a.T, do, preferred_element_type=jnp.float32)
        da = jnp.dot(do, a2.T, preferred_element_type=jnp.float32)
        du = (da * v * sg * (1.0 + u * (1.0 - sg))).astype(jnp.bfloat16)
        dv = (da * u * sg).astype(jnp.bfloat16)
        gw1 = jnp.dot(xs.T, du, preferred_element_type=jnp.float32)
        gw3 = jnp.dot(xs.T, dv, preferred_element_type=jnp.float32)
        dxs = jnp.dot(du, a1.T, preferred_element_type=jnp.float32) + jnp.dot(dv, a3.T, preferred_element_type=jnp.float32)
        dx_acc = dx_acc.at[tk].add(dxs.astype(jnp.bfloat16).astype(jnp.float32))
        return (y_acc, dx_acc, dg), (gw1, gw3, gw2)

    init = (jnp.zeros((TG, D), jnp.float32), jnp.zeros((TG, D), jnp.float32), jnp.zeros((n,), jnp.float32))
    (y_acc, dx_acc, dg), (gw1, gw3, gw2) = lax.scan(body, init, (tab, w1, w3, w2))
    return (y_acc.astype(jnp.bfloat16), dx_acc.astype(jnp.bfloat16), dg.reshape(TG, TOP), gw1, gw3, gw2)
```

```python
import functools

import jax
import jax.numpy as jnp
from jax import lax
from jax.experimental import pallas as pl
from jax.experimental.pallas import tpu as pltpu
from jax.sharding import PartitionSpec as P

ND = 8
CAP = 24
BF = jnp.bfloat16
F32 = jnp.float32
VMEM_LIMIT = 60 * 1024 * 1024


def dot(a, b):
    return jnp.dot(a, b, preferred_element_type=F32)


def dot_nt(a, b):
    return lax.dot_general(a, b, (((1,), (1,)), ((), ())), preferred_element_type=F32)


def dot_tn(a, b):
    return lax.dot_general(a, b, (((0,), (0,)), ((), ())), preferred_element_type=F32)


def params(n=1):
    return pltpu.CompilerParams(dimension_semantics=("arbitrary",) * n, vmem_limit_bytes=VMEM_LIMIT)


def cost(flops, nbytes):
    return pl.CostEstimate(flops=int(flops), bytes_accessed=int(nbytes), transcendentals=0)


def whole(shape):
    return pl.BlockSpec(shape, lambda *_: (0,) * len(shape))


def select_rows(rank, el):
    r = lax.broadcasted_iota(jnp.int32, (CAP, rank.shape[1]), 0).astype(F32)
    return jnp.concatenate([jnp.where(rank[e:e + 1, :] == r, 1.0, 0.0) for e in range(el)], axis=0)


def expand_rows(mat, el):
    return jnp.concatenate([jnp.broadcast_to(mat[e:e + 1, :], (CAP, mat.shape[1])) for e in range(el)], axis=0)


def split3(g):
    hi = g.astype(BF)
    rest = g - hi.astype(F32)
    mid = rest.astype(BF)
    low = (rest - mid.astype(F32)).astype(BF)
    return hi, mid, low


def route_kernel(p_ref, meta_ref, rank_ref, gate_ref, *, el, top):
    p = p_ref[0]
    tok = meta_ref.shape[2]
    ep = rank_ref.shape[1]
    eid = (lax.broadcasted_iota(jnp.int32, (ep, tok), 0) + p * el).astype(F32)
    live = lax.broadcasted_iota(jnp.int32, (ep, tok), 0) < el
    before = (lax.broadcasted_iota(jnp.int32, (tok, tok), 0) < lax.broadcasted_iota(jnp.int32, (tok, tok), 1))
    before = jnp.where(before, 1.0, 0.0).astype(BF)
    for s in range(ND):
        m = meta_ref[p ^ s]
        hit = jnp.zeros((ep, tok), F32)
        gate = jnp.zeros((ep, tok), F32)
        for j in range(top):
            same = (m[j:j + 1, :] == eid) & live
            hit = hit + jnp.where(same, 1.0, 0.0)
            gate = gate + jnp.where(same, m[8 + j:9 + j, :], 0.0)
        rank = dot(hit.astype(BF), before)
        rank_ref[s] = jnp.where(hit > 0.0, rank, -1.0)
        gate_ref[s] = gate


def gather_experts(rank_ref, srcs, out_ref, el, gate_ref=None):
    d = srcs[0].shape[1]
    step = 256
    for q in range(ND // 2):
        sel = [select_rows(rank_ref[2 * q + h], el) for h in range(2)]
        if gate_ref is not None:
            g = [jnp.sum(sel[h] * expand_rows(gate_ref[2 * q + h], el), axis=1, keepdims=True) for h in range(2)]
        sel = [m.astype(BF) for m in sel]
        for n in range(0, d, step):
            rows = [dot(sel[h], srcs[2 * q + h][:, n:n + step]) for h in range(2)]
            if gate_ref is not None:
                rows = [rows[h] * g[h] for h in range(2)]
            for e in range(el):
                part = jnp.concatenate([rows[h][e * CAP:(e + 1) * CAP] for h in range(2)], axis=0)
                out_ref[e, 2 * q * CAP:(2 * q + 2) * CAP, n:n + step] = part.astype(BF)


def up_kernel(rank_ref, *refs, el):
    srcs = refs[:ND]
    w1_ref, w3_ref, u_ref, v_ref, a_ref, xs_ref = refs[ND:]
    e = pl.program_id(0)

    @pl.when(e == 0)
    def _():
        gather_experts(rank_ref, srcs, xs_ref, el)

    xs = xs_ref[e]
    u = dot(xs, w1_ref[0]).astype(BF)
    v = dot(xs, w3_ref[0]).astype(BF)
    uf = u.astype(F32)
    u_ref[0] = u
    v_ref[0] = v
    a_ref[0] = (uf * jax.nn.sigmoid(uf) * v.astype(F32)).astype(BF)


def to_sources(rows, out_ref):
    for s in range(ND):
        part = jnp.concatenate([r[s * CAP:(s + 1) * CAP] for r in rows], axis=0)
        out_ref[s] = part.astype(BF)


def down_kernel(a_ref, w2_ref, o_ref):
    to_sources([dot(a_ref[h], w2_ref[h]) for h in range(2)], o_ref)


def combine_y_kernel(p_ref, rank_ref, gate_ref, o_ref, dy_ref, send_ref, keep_ref, dg_ref, *, el):
    i = pl.program_id(0)
    sel = select_rows(rank_ref[0], el)
    gexp = expand_rows(gate_ref[0], el)
    o = o_ref[0]
    y = None
    for piece in split3(sel * gexp):
        part = dot_tn(piece, o)
        y = part if y is None else y + part

    @pl.when(i < ND // 2)
    def _():
        send_ref[0] = y

    @pl.when(i >= ND // 2)
    def _():
        keep_ref[0] = y

    dys = dot(sel.astype(BF), dy_ref[0])
    dg = jnp.sum(dys * o.astype(F32), axis=1, keepdims=True)
    spread = sel * dg
    rows = [jnp.sum(spread[e * CAP:(e + 1) * CAP], axis=0, keepdims=True) for e in range(el)]
    rows.append(jnp.zeros((dg_ref.shape[1] - el, sel.shape[1]), F32))
    dg_ref[0] = jnp.concatenate(rows, axis=0)


def combine_dx_kernel(rank_ref, o_ref, send_ref, keep_ref, *, el):
    i = pl.program_id(0)
    dx = dot_tn(select_rows(rank_ref[0], el).astype(BF), o_ref[0])

    @pl.when(i < ND // 2)
    def _():
        send_ref[0] = dx

    @pl.when(i >= ND // 2)
    def _():
        keep_ref[0] = dx


def act_kernel(rank_ref, gate_ref, *refs, el):
    srcs = refs[:ND]
    w2_ref, u_ref, v_ref, a_ref, du_ref, dv_ref, gw2_ref, do_ref = refs[ND:]
    e = pl.program_id(0)

    @pl.when(e == 0)
    def _():
        gather_experts(rank_ref, srcs, do_ref, el, gate_ref)

    do = do_ref[e]
    gw2_ref[0] = dot_tn(a_ref[0], do)
    da = dot_nt(do, w2_ref[0])
    u = u_ref[0].astype(F32)
    v = v_ref[0].astype(F32)
    sg = jax.nn.sigmoid(u)
    du_ref[0] = (da * v * sg * (1.0 + u * (1.0 - sg))).astype(BF)
    dv_ref[0] = (da * u * sg).astype(BF)


def dx_kernel(du_ref, dv_ref, w1_ref, w3_ref, o_ref):
    to_sources([dot_nt(du_ref[h], w1_ref[h]) + dot_nt(dv_ref[h], w3_ref[h]) for h in range(2)], o_ref)


def grad_kernel(rank_ref, *refs, el):
    srcs = refs[:ND]
    du_ref, dv_ref, gw1_ref, gw3_ref, xs_ref = refs[ND:]
    e = pl.program_id(0)

    @pl.when(e == 0)
    def _():
        gather_experts(rank_ref, srcs, xs_ref, el)

    xs = xs_ref[e]
    gw1_ref[0] = dot_tn(xs, du_ref[0])
    gw3_ref[0] = dot_tn(xs, dv_ref[0])


def solution(mesh):
    grp = ('row', 'col')
    tspec = P(('dp', 'row', 'col'), None)
    wspec = P(grp, None, None)
    gspec = P(('dp', 'row', 'col'), None, None)

    def permute(a, k):
        return lax.ppermute(a, grp, [(p, p ^ k) for p in range(ND)])

    def gather_tokens(a):
        got = {0: a, 1: permute(a, 1)}
        for k in (2, 4, 6):
            got[k] = permute(a, k)
        for k in (2, 4, 6):
            got[k + 1] = permute(got[k], 1)
        return [got[k] for k in range(ND)]

    def return_sums(send, keep):
        got = permute(send, 1)
        total = keep[0] + got[0]
        for k in range(1, ND // 2):
            total = total + permute(keep[k] + got[k], 2 * k)
        return total.astype(BF)

    def local(x, ridx, gates, w1, w3, w2, dy):
        tok, d = x.shape
        top = ridx.shape[1]
        el, _, ff = w1.shape
        ep = -(-el // 8) * 8
        m = ND * CAP
        rows = el * CAP
        p = (lax.axis_index('row') * mesh.shape['col'] + lax.axis_index('col')).astype(jnp.int32).reshape(1)
        pad = jnp.zeros((8 - top, tok), F32)
        meta = jnp.concatenate([ridx.T.astype(F32), pad, gates.T, pad])
        meta = lax.all_gather(meta, grp)
        xg = gather_tokens(x)
        dyg = gather_tokens(dy)
        smem = pl.BlockSpec(memory_space=pltpu.SMEM)
        sd = jax.ShapeDtypeStruct
        rank, gate = pl.pallas_call(
            functools.partial(route_kernel, el=el, top=top),
            in_specs=[smem, pl.BlockSpec(memory_space=pltpu.VMEM)],
            out_shape=[sd((ND, ep, tok), F32)] * 2,
            name='route')(p, meta)

        tab = whole((ND, ep, tok))
        srcs = [whole((tok, d))] * ND

        def per(shape):
            return pl.BlockSpec((1,) + shape, lambda e: (e,) + (0,) * len(shape))

        def per2(shape):
            return pl.BlockSpec((2,) + shape, lambda e: (e,) + (0,) * len(shape))

        prod = 2.0 * el * m * d * ff
        wb = el * d * ff * 2
        hid = sd((el, m, ff), BF)
        u, v, a = pl.pallas_call(
            functools.partial(up_kernel, el=el), grid=(el,),
            in_specs=[tab] + srcs + [per((d, ff))] * 2,
            out_specs=[per((m, ff))] * 3,
            out_shape=[hid] * 3,
            scratch_shapes=[pltpu.VMEM((el, m, d), BF)],
            compiler_params=params(), cost_estimate=cost(2 * prod, 2 * wb), name='up')(rank, *xg, w1, w3)

        by_src = pl.BlockSpec((ND, 2 * CAP, d), lambda e: (0, e, 0))
        o = pl.pallas_call(
            down_kernel, grid=(el // 2,),
            in_specs=[per2((m, ff)), per2((ff, d))],
            out_specs=by_src,
            out_shape=sd((ND, rows, d), BF),
            compiler_params=params(), cost_estimate=cost(prod, wb), name='down')(a, w2)

        half = ND // 2

        def src_of(i):
            return jnp.where(i < half, 2 * i + 1, 2 * (i - half))

        def src(shape):
            return pl.BlockSpec((1,) + shape, lambda i, *_: (src_of(i),) + (0,) * len(shape))

        send_spec = pl.BlockSpec((1, tok, d), lambda i, *_: (jnp.minimum(i, half - 1), 0, 0))
        keep_spec = pl.BlockSpec((1, tok, d), lambda i, *_: (jnp.maximum(i - half, 0), 0, 0))
        sums = [sd((half, tok, d), F32)] * 2
        ysend, ykeep, dg = pl.pallas_call(
            functools.partial(combine_y_kernel, el=el),
            grid_spec=pltpu.PrefetchScalarGridSpec(
                num_scalar_prefetch=1, grid=(ND,),
                in_specs=[src((ep, tok))] * 2 + [src((rows, d)), src((tok, d))],
                out_specs=[send_spec, keep_spec,
                           pl.BlockSpec((1, ep, tok), lambda i, pr: (pr[0] ^ src_of(i), 0, 0))]),
            out_shape=sums + [sd((ND, ep, tok), F32)],
            compiler_params=params(), cost_estimate=cost(8.0 * ND * rows * tok * d, 2 * ND * rows * d),
            name='combine_y')(p, rank, gate, o, jnp.stack(dyg))

        y = return_sums(ysend, ykeep)

        du, dv, gw2 = pl.pallas_call(
            functools.partial(act_kernel, el=el), grid=(el,),
            in_specs=[tab] * 2 + srcs + [per((ff, d))] + [per((m, ff))] * 3,
            out_specs=[per((m, ff))] * 2 + [per((ff, d))],
            out_shape=[hid] * 2 + [sd((el, ff, d), F32)],
            scratch_shapes=[pltpu.VMEM((el, m, d), BF)],
            compiler_params=params(), cost_estimate=cost(2 * prod, 3 * wb), name='act')(
                rank, gate, *dyg, w2, u, v, a)

        dxo = pl.pallas_call(
            dx_kernel, grid=(el // 2,),
            in_specs=[per2((m, ff))] * 2 + [per2((d, ff))] * 2,
            out_specs=by_src,
            out_shape=sd((ND, rows, d), BF),
            compiler_params=params(), cost_estimate=cost(2 * prod, 2 * wb), name='dx')(du, dv, w1, w3)

        xsend, xkeep = pl.pallas_call(
            functools.partial(combine_dx_kernel, el=el), grid=(ND,),
            in_specs=[src((ep, tok)), src((rows, d))],
            out_specs=[send_spec, keep_spec],
            out_shape=sums,
            compiler_params=params(), cost_estimate=cost(2.0 * ND * rows * tok * d, 2 * ND * rows * d),
            name='combine_dx')(rank, dxo)
        dx = return_sums(xsend, xkeep)

        gw1, gw3 = pl.pallas_call(
            functools.partial(grad_kernel, el=el), grid=(el,),
            in_specs=[tab] + srcs + [per((m, ff))] * 2,
            out_specs=[per((d, ff))] * 2,
            out_shape=[sd((el, d, ff), F32)] * 2,
            scratch_shapes=[pltpu.VMEM((el, m, d), BF)],
            compiler_params=params(), cost_estimate=cost(2 * prod, 4 * wb), name='grad')(rank, *xg, du, dv)

        dgall = lax.all_to_all(dg, grp, 0, 0, tiled=True)[:, :el].reshape(ND * el, tok).T
        pick = ridx[:, :, None] == jnp.arange(ND * el, dtype=jnp.int32)
        dgates = jnp.sum(jnp.where(pick, dgall[:, None, :], 0.0), axis=2)
        return y, dx, dgates, gw1, gw3, gw2

    return jax.shard_map(local, mesh=mesh, in_specs=(tspec, tspec, tspec, wspec, wspec, wspec, tspec),
                         out_specs=(tspec, tspec, tspec, gspec, gspec, gspec), check_vma=False)
```

```python
import functools

import jax
import jax.numpy as jnp
from jax import lax
from jax.experimental import pallas as pl
from jax.experimental.pallas import tpu as pltpu
from jax.sharding import PartitionSpec as P


ND = 8
CAP = 24
BF = jnp.bfloat16
F32 = jnp.float32
VMEM_LIMIT = 60 * 1024 * 1024
MESH = pl.DeviceIdType.MESH


def dot(a, b):
    return jnp.dot(a, b, preferred_element_type=F32)


def dot_nt(a, b):
    return lax.dot_general(a, b, (((1,), (1,)), ((), ())), preferred_element_type=F32)


def dot_tn(a, b):
    return lax.dot_general(a, b, (((0,), (0,)), ((), ())), preferred_element_type=F32)


def params(n=1):
    return pltpu.CompilerParams(dimension_semantics=("arbitrary",) * n, vmem_limit_bytes=VMEM_LIMIT)


def cost(flops, nbytes):
    return pl.CostEstimate(flops=int(flops), bytes_accessed=int(nbytes), transcendentals=0)


def select_rows(rank, el):
    r = lax.broadcasted_iota(jnp.int32, (CAP, rank.shape[1]), 0).astype(F32)
    return jnp.concatenate([jnp.where(rank[e:e + 1, :] == r, 1.0, 0.0) for e in range(el)], axis=0)


def expand_rows(mat, el):
    return jnp.concatenate([jnp.broadcast_to(mat[e:e + 1, :], (CAP, mat.shape[1])) for e in range(el)], axis=0)


def split3(g):
    hi = g.astype(BF)
    rest = g - hi.astype(F32)
    mid = rest.astype(BF)
    low = (rest - mid.astype(F32)).astype(BF)
    return hi, mid, low


def peer(k, ncol):
    p = lax.axis_index('row') * ncol + lax.axis_index('col')
    q = p ^ k
    return {'row': q // ncol, 'col': q % ncol}


def share_kernel(meta_ref, x_ref, dy_ref, xg_ref, dyg_ref, rank_ref, gate_ref, metas, send_sem, recv_sem, meta_send,
                 meta_recv, own_sem, *, el, top, ncol):
    barrier = pltpu.get_barrier_semaphore()
    for k in range(1, ND):
        pl.semaphore_signal(barrier, inc=1, device_id=peer(k, ncol), device_id_type=MESH)
    pl.semaphore_wait(barrier, ND - 1)

    def remote(src, dst, ss, rs, k):
        return pltpu.make_async_remote_copy(src_ref=src, dst_ref=dst, send_sem=ss, recv_sem=rs,
                                            device_id=peer(k, ncol), device_id_type=MESH)

    small = [remote(meta_ref, metas.at[k], meta_send.at[k], meta_recv.at[k], k) for k in range(1, ND)]
    for c in small:
        c.start()
    outs = (xg_ref, dyg_ref)
    ins = (x_ref, dy_ref)
    sends = {}
    for b in range(2):
        for k in (6, 2, 4, 1):
            sends[b, k] = remote(ins[b], outs[b].at[k], send_sem.at[b, k], recv_sem.at[b, k], k)
            sends[b, k].start()
    own = [pltpu.make_async_copy(ins[b], outs[b].at[0], own_sem.at[b]) for b in range(2)]
    for c in own:
        c.start()
    for c in small:
        c.wait()

    tok = meta_ref.shape[1]
    ep = rank_ref.shape[1]
    p = lax.axis_index('row') * ncol + lax.axis_index('col')
    eid = (lax.broadcasted_iota(jnp.int32, (ep, tok), 0) + p * el).astype(F32)
    live = lax.broadcasted_iota(jnp.int32, (ep, tok), 0) < el
    before = (lax.broadcasted_iota(jnp.int32, (tok, tok), 0) < lax.broadcasted_iota(jnp.int32, (tok, tok), 1))
    before = jnp.where(before, 1.0, 0.0).astype(BF)
    for s in range(ND):
        m = meta_ref[...] if s == 0 else metas[s]
        hit = jnp.zeros((ep, tok), F32)
        gate = jnp.zeros((ep, tok), F32)
        for j in range(top):
            same = (m[j:j + 1, :] == eid) & live
            hit = hit + jnp.where(same, 1.0, 0.0)
            gate = gate + jnp.where(same, m[8 + j:9 + j, :], 0.0)
        rank = dot(hit.astype(BF), before)
        rank_ref[s] = jnp.where(hit > 0.0, rank, -1.0)
        gate_ref[s] = gate

    for b in range(2):
        for k in (2, 4, 6):
            sends[b, k].wait_recv()
            sends[b, k + 1] = remote(outs[b].at[k], outs[b].at[k + 1], send_sem.at[b, k + 1], recv_sem.at[b, k + 1], 1)
            sends[b, k + 1].start()
    for b in range(2):
        for k in (1, 3, 5, 7):
            sends[b, k].wait_recv()
        for k in range(1, ND):
            sends[b, k].wait_send()
    for c in own:
        c.wait()


def gather_pair(rank_ref, src_ref, i, gate_ref=None):
    parts = []
    for s in range(ND):
        rank = rank_ref[s, pl.ds(2 * i, 2), :]
        sel = select_rows(rank, 2)
        rows = dot(sel.astype(BF), src_ref[s])
        if gate_ref is not None:
            gate = expand_rows(gate_ref[s, pl.ds(2 * i, 2), :], 2)
            rows = rows * jnp.sum(sel * gate, axis=1, keepdims=True)
        parts.append(rows)
    return [jnp.concatenate([r[h * CAP:(h + 1) * CAP] for r in parts], axis=0).astype(BF) for h in range(2)]


def to_sources(rows, out_ref, i):
    for s in range(ND):
        part = jnp.concatenate([r[s * CAP:(s + 1) * CAP] for r in rows], axis=0)
        out_ref[s, pl.ds(pl.multiple_of(i * 2 * CAP, 16), 2 * CAP), :] = part.astype(BF)


def source_of(j):
    return jnp.where(j < ND // 2, 2 * j + 1, 2 * (j - ND // 2))


def forward_kernel(p_ref, rank_ref, gate_ref, x_ref, dy_ref, w1_ref, w3_ref, w2_ref, u_ref, v_ref, send_ref, keep_ref,
                   dg_ref, o_ref, *, el):
    i = pl.program_id(0)
    steps = el // 2

    @pl.when(i < steps)
    def _():
        outs = []
        for h, xs in enumerate(gather_pair(rank_ref, x_ref, i)):
            uv = dot(xs, jnp.concatenate([w1_ref[h], w3_ref[h]], axis=1)).astype(BF)
            ff = uv.shape[1] // 2
            u, v = uv[:, :ff], uv[:, ff:]
            u_ref[h] = u
            v_ref[h] = v
            uf = u.astype(F32)
            a = (uf * jax.nn.sigmoid(uf) * v.astype(F32)).astype(BF)
            outs.append(dot(a, w2_ref[h]))
        to_sources(outs, o_ref, i)

    @pl.when(i >= steps)
    def _():
        j = i - steps
        s = source_of(j)
        sel = select_rows(rank_ref[s], el)
        gexp = expand_rows(gate_ref[s], el)
        o = o_ref[s]
        y = None
        for piece in split3(jnp.transpose(sel * gexp)):
            part = dot(piece, o)
            y = part if y is None else y + part

        @pl.when(j < ND // 2)
        def _():
            send_ref[0] = y

        @pl.when(j >= ND // 2)
        def _():
            keep_ref[0] = y

        dys = dot(sel.astype(BF), dy_ref[s])
        dg = jnp.sum(dys * o.astype(F32), axis=1, keepdims=True)
        spread = sel * dg
        rows = [jnp.sum(spread[e * CAP:(e + 1) * CAP], axis=0, keepdims=True) for e in range(el)]
        rows.append(jnp.zeros((dg_ref.shape[1] - el, sel.shape[1]), F32))
        dg_ref[0] = jnp.concatenate(rows, axis=0)


def backward_kernel(rank_ref, gate_ref, dy_ref, w1_ref, w3_ref, w2_ref, u_ref, v_ref, du_ref, dv_ref, send_ref,
                    keep_ref, o_ref, *, el):
    i = pl.program_id(0)
    steps = el // 2

    @pl.when(i < steps)
    def _():
        outs = []
        for h, do in enumerate(gather_pair(rank_ref, dy_ref, i, gate_ref)):
            da = dot_nt(do, w2_ref[h])
            u = u_ref[h].astype(F32)
            v = v_ref[h].astype(F32)
            sg = jax.nn.sigmoid(u)
            du = (da * v * sg * (1.0 + u * (1.0 - sg))).astype(BF)
            dv = (da * u * sg).astype(BF)
            du_ref[h] = du
            dv_ref[h] = dv
            outs.append(dot_nt(jnp.concatenate([du, dv], axis=1), jnp.concatenate([w1_ref[h], w3_ref[h]], axis=1)))
        to_sources(outs, o_ref, i)

    @pl.when(i >= steps)
    def _():
        j = i - steps
        s = source_of(j)
        dx = dot(jnp.transpose(select_rows(rank_ref[s], el)).astype(BF), o_ref[s])

        @pl.when(j < ND // 2)
        def _():
            send_ref[0] = dx

        @pl.when(j >= ND // 2)
        def _():
            keep_ref[0] = dx


def grad_kernel(rank_ref, gate_ref, x_ref, dy_ref, u_ref, v_ref, du_ref, dv_ref, gw1_ref, gw3_ref, gw2_ref):
    i = pl.program_id(0)
    dos = gather_pair(rank_ref, dy_ref, i, gate_ref)
    for h, xs in enumerate(gather_pair(rank_ref, x_ref, i)):
        gw1_ref[h] = dot_tn(xs, du_ref[h])
        gw3_ref[h] = dot_tn(xs, dv_ref[h])
        u = u_ref[h].astype(F32)
        a = (u * jax.nn.sigmoid(u) * v_ref[h].astype(F32)).astype(BF)
        gw2_ref[h] = dot_tn(a, dos[h])


def solution(mesh):
    grp = ('row', 'col')
    tspec = P(('dp', 'row', 'col'), None)
    wspec = P(grp, None, None)
    gspec = P(('dp', 'row', 'col'), None, None)
    ncol = mesh.shape['col']

    def permute(a, k):
        return lax.ppermute(a, grp, [(p, p ^ k) for p in range(ND)])

    def return_sums(send, keep):
        got = permute(send, 1)
        total = keep[0] + got[0]
        for k in range(1, ND // 2):
            total = total + permute(keep[k] + got[k], 2 * k)
        return total.astype(BF)

    def body(x, ridx, gates, w1, w3, w2, dy):
        tok, d = x.shape
        top = ridx.shape[1]
        el, _, ff = w1.shape
        ep = -(-el // 8) * 8
        m = ND * CAP
        rows = el * CAP
        steps = el // 2
        half = ND // 2
        p = (lax.axis_index('row') * ncol + lax.axis_index('col')).astype(jnp.int32).reshape(1)
        pad = jnp.zeros((8 - top, tok), F32)
        meta = jnp.concatenate([ridx.T.astype(F32), pad, gates.T, pad])
        sd = jax.ShapeDtypeStruct
        vmem = pl.BlockSpec(memory_space=pltpu.VMEM)
        dma = pltpu.SemaphoreType.DMA
        xg, dyg, rank, gate = pl.pallas_call(
            functools.partial(share_kernel, el=el, top=top, ncol=ncol),
            in_specs=[vmem] * 3, out_specs=[vmem] * 4,
            out_shape=[sd((ND, tok, d), BF)] * 2 + [sd((ND, ep, tok), F32)] * 2,
            scratch_shapes=[pltpu.VMEM((ND,) + meta.shape, F32), dma((2, ND)), dma((2, ND)), dma((ND,)), dma((ND,)),
                            dma((2,))],
            compiler_params=pltpu.CompilerParams(collective_id=0, has_side_effects=True, vmem_limit_bytes=VMEM_LIMIT),
            name='share')(meta, x, dy)

        def once(shape):
            return pl.BlockSpec(shape, lambda *_: (0,) * len(shape), pipeline_mode=pl.Buffered(1))

        def pair(shape):
            return pl.BlockSpec((2,) + shape, lambda i, *_: (jnp.minimum(i, steps - 1),) + (0,) * len(shape))

        tabs = [once((ND, ep, tok))] * 2
        toks = once((ND, tok, d))
        ups = pair((d, ff))
        downs = pair((ff, d))
        hids = pair((m, ff))
        prod = 2.0 * el * m * d * ff
        wb = el * d * ff * 2
        hid = sd((el, m, ff), BF)
        send_spec = pl.BlockSpec((1, tok, d), lambda i, *_: (jnp.clip(i - steps, 0, half - 1), 0, 0))
        keep_spec = pl.BlockSpec((1, tok, d), lambda i, *_: (jnp.maximum(i - steps - half, 0), 0, 0))
        sums = [sd((half, tok, d), F32)] * 2
        kept = pltpu.VMEM((ND, rows, d), BF)

        u, v, ysend, ykeep, dg = pl.pallas_call(
            functools.partial(forward_kernel, el=el),
            grid_spec=pltpu.PrefetchScalarGridSpec(
                num_scalar_prefetch=1, grid=(steps + ND,),
                in_specs=tabs + [toks] * 2 + [ups] * 2 + [downs],
                out_specs=[hids] * 2 + [send_spec, keep_spec, pl.BlockSpec(
                    (1, ep, tok), lambda i, pr: (pr[0] ^ source_of(jnp.maximum(i - steps, 0)), 0, 0))],
                scratch_shapes=[kept]),
            out_shape=[hid] * 2 + sums + [sd((ND, ep, tok), F32)],
            compiler_params=params(), cost_estimate=cost(3 * prod, 3 * wb), name='forward')(
                p, rank, gate, xg, dyg, w1, w3, w2)
        y = return_sums(ysend, ykeep)

        du, dv, xsend, xkeep = pl.pallas_call(
            functools.partial(backward_kernel, el=el), grid=(steps + ND,),
            in_specs=tabs + [toks] + [ups] * 2 + [downs] + [hids] * 2,
            out_specs=[hids] * 2 + [send_spec, keep_spec],
            out_shape=[hid] * 2 + sums,
            scratch_shapes=[kept],
            compiler_params=params(), cost_estimate=cost(3 * prod, 3 * wb), name='backward')(
                rank, gate, dyg, w1, w3, w2, u, v)
        dx = return_sums(xsend, xkeep)

        gw1, gw3, gw2 = pl.pallas_call(
            grad_kernel, grid=(steps,),
            in_specs=tabs + [toks] * 2 + [hids] * 4,
            out_specs=[ups] * 2 + [downs],
            out_shape=[sd((el, d, ff), F32)] * 2 + [sd((el, ff, d), F32)],
            compiler_params=params(), cost_estimate=cost(3 * prod, 6 * wb), name='grad')(
                rank, gate, xg, dyg, u, v, du, dv)

        dgall = lax.all_to_all(dg, grp, 0, 0, tiled=True)[:, :el].reshape(ND * el, tok).T
        pick = ridx[:, :, None] == jnp.arange(ND * el, dtype=jnp.int32)
        dgates = jnp.sum(jnp.where(pick, dgall[:, None, :], 0.0), axis=2)
        return y, dx, dgates, gw1, gw3, gw2

    return jax.shard_map(body, mesh=mesh, in_specs=(tspec, tspec, tspec, wspec, wspec, wspec, tspec),
                         out_specs=(tspec, tspec, tspec, gspec, gspec, gspec), check_vma=False)
```

```python
import functools

import jax
import jax.numpy as jnp
from jax import lax
from jax.experimental import pallas as pl
from jax.experimental.pallas import tpu as pltpu
from jax.sharding import PartitionSpec as P


ND = 8
CAP = 24
BF = jnp.bfloat16
F32 = jnp.float32
VMEM_LIMIT = 60 * 1024 * 1024
MESH = pl.DeviceIdType.MESH


def dot(a, b):
    return jnp.dot(a, b, preferred_element_type=F32)


def dot_nt(a, b):
    return lax.dot_general(a, b, (((1,), (1,)), ((), ())), preferred_element_type=F32)


def dot_tn(a, b):
    return lax.dot_general(a, b, (((0,), (0,)), ((), ())), preferred_element_type=F32)


def params(n=1):
    return pltpu.CompilerParams(dimension_semantics=("arbitrary",) * n, vmem_limit_bytes=VMEM_LIMIT)


def cost(flops, nbytes):
    return pl.CostEstimate(flops=int(flops), bytes_accessed=int(nbytes), transcendentals=0)


def select_rows(rank, el):
    r = lax.broadcasted_iota(jnp.int32, (CAP, rank.shape[1]), 0).astype(F32)
    return jnp.concatenate([jnp.where(rank[e:e + 1, :] == r, 1.0, 0.0) for e in range(el)], axis=0)


def expand_rows(mat, el):
    return jnp.concatenate([jnp.broadcast_to(mat[e:e + 1, :], (CAP, mat.shape[1])) for e in range(el)], axis=0)


def split3(g):
    hi = g.astype(BF)
    rest = g - hi.astype(F32)
    mid = rest.astype(BF)
    low = (rest - mid.astype(F32)).astype(BF)
    return hi, mid, low


def peer(k, ncol):
    p = lax.axis_index('row') * ncol + lax.axis_index('col')
    q = p ^ k
    return {'row': q // ncol, 'col': q % ncol}


def gather_pair(rank_ref, src_ref, i, gate_ref=None):
    parts = []
    for s in range(ND):
        rank = rank_ref[s, pl.ds(2 * i, 2), :]
        sel = select_rows(rank, 2)
        rows = dot(sel.astype(BF), src_ref[s])
        if gate_ref is not None:
            gate = expand_rows(gate_ref[s, pl.ds(2 * i, 2), :], 2)
            rows = rows * jnp.sum(sel * gate, axis=1, keepdims=True)
        parts.append(rows)
    return [jnp.concatenate([r[h * CAP:(h + 1) * CAP] for r in parts], axis=0).astype(BF) for h in range(2)]


def to_sources(rows, out_ref, i):
    for s in range(ND):
        part = jnp.concatenate([r[s * CAP:(s + 1) * CAP] for r in rows], axis=0)
        out_ref[s, pl.ds(pl.multiple_of(i * 2 * CAP, 16), 2 * CAP), :] = part.astype(BF)


def block_of(j):
    return (j + 1) % (ND // 2)


def layer_kernel(ids_ref, gates_ref, x_ref, dy_ref, w1_ref, w3_ref, w2_ref,
                 u_ref, v_ref, du_ref, dv_ref, x0_ref, x1_ref, x2_ref, x3_ref, y_ref, dg_ref,
                 xg_out, dyg_out, rank_out, gate_out,
                 xg, dyg, rank_s, gate_s, ids_s, gates_s, us, vs, rows_s, ysend, yrecv, ytot, ychip, xsend, xrecv,
                 dgs, dgr, ids_sem, gates_sem, tok_sem, yd_sem, yc_sem, xd_sem, dg_sem, out_sem, *, el, ncol):
    i = pl.program_id(0)
    steps = el // 2
    half = ND // 2
    t_y, t_b, t_x = steps, steps + ND, 2 * steps + ND
    last = t_x + ND - 1
    top, tok = ids_ref.shape
    ep = rank_s.shape[1]
    p = lax.axis_index('row') * ncol + lax.axis_index('col')

    def remote(src, dst, sem, n, k):
        return pltpu.make_async_remote_copy(src_ref=src, dst_ref=dst, send_sem=sem.at[(0,) + n],
                                            recv_sem=sem.at[(1,) + n], device_id=peer(k, ncol), device_id_type=MESH)

    def ids_copy(k):
        return remote(ids_ref, ids_s.at[k], ids_sem, (k,), k)

    def gates_copy(k):
        return remote(gates_ref, gates_s.at[k], gates_sem, (k,), k)

    def tok_copy(b, k):
        buf = (xg, dyg)[b]
        if k in (3, 5, 7):
            return remote(buf.at[k - 1], buf.at[k], tok_sem, (b, k), 1)
        return remote((x_ref, dy_ref)[b], buf.at[k], tok_sem, (b, k), k)

    def y_core(d):
        return remote(ysend.at[d], yrecv.at[d], yd_sem, (d,), 1)

    def y_chip(d):
        return remote(ytot.at[d], ychip.at[d], yc_sem, (d,), 2 * d)

    def x_core(d):
        return remote(xsend.at[d], xrecv.at[d], xd_sem, (d,), 1)

    def dg_copy(k):
        return remote(dgs.at[k], dgr.at[k], dg_sem, (k,), k)

    outs = ((xg, xg_out), (dyg, dyg_out), (rank_s, rank_out), (gate_s, gate_out))

    def out_copy(n):
        return pltpu.make_async_copy(outs[n][0], outs[n][1], out_sem.at[n])

    @pl.when(i == 0)
    def _():
        barrier = pltpu.get_barrier_semaphore()
        for k in range(1, ND):
            pl.semaphore_signal(barrier, inc=1, device_id=peer(k, ncol), device_id_type=MESH)
        pl.semaphore_wait(barrier, ND - 1)
        for k in range(1, ND):
            ids_copy(k).start()
            gates_copy(k).start()
        for b in range(2):
            for k in (6, 2, 4, 1):
                tok_copy(b, k).start()
        xg[0] = x_ref[...]
        dyg[0] = dy_ref[...]
        for k in range(1, ND):
            ids_copy(k).wait()
            gates_copy(k).wait()
        first = lax.broadcasted_iota(jnp.int32, (ep, tok), 0)
        eid = first + p * el
        live = first < el
        before = lax.broadcasted_iota(jnp.int32, (tok, tok), 0) < lax.broadcasted_iota(jnp.int32, (tok, tok), 1)
        before = jnp.where(before, 1.0, 0.0).astype(BF)
        for s in range(ND):
            ids = ids_ref[...] if s == 0 else ids_s[s]
            gat = gates_ref[...] if s == 0 else gates_s[s]
            hit = jnp.zeros((ep, tok), F32)
            gate = jnp.zeros((ep, tok), F32)
            for j in range(top):
                same = (ids[j:j + 1, :] == eid) & live
                hit = hit + jnp.where(same, 1.0, 0.0)
                gate = gate + jnp.where(same, gat[j:j + 1, :], 0.0)
            rank = dot(hit.astype(BF), before)
            rank_s[s] = jnp.where(hit > 0.0, rank, -1.0)
            gate_s[s] = gate
        for k in (2, 4, 6):
            tok_copy(0, k).wait_recv()
            tok_copy(0, k + 1).start()
        for k in (1, 3, 5, 7):
            tok_copy(0, k).wait_recv()

    @pl.when(i == t_y - 3)
    def _():
        for k in (2, 4, 6):
            tok_copy(1, k).wait_recv()
            tok_copy(1, k + 1).start()

    @pl.when(i == t_y)
    def _():
        for k in (1, 3, 5, 7):
            tok_copy(1, k).wait_recv()
        for n in range(4):
            out_copy(n).start()

    @pl.when(i < t_y)
    def _():
        res = []
        for h, xs in enumerate(gather_pair(rank_s, xg, i)):
            uv = dot(xs, jnp.concatenate([w1_ref[h], w3_ref[h]], axis=1)).astype(BF)
            ff = uv.shape[1] // 2
            u, v = uv[:, :ff], uv[:, ff:]
            u_ref[h] = u
            v_ref[h] = v
            us[2 * i + h] = u
            vs[2 * i + h] = v
            uf = u.astype(F32)
            a = (uf * jax.nn.sigmoid(uf) * v.astype(F32)).astype(BF)
            res.append(dot(a, w2_ref[h]))
        to_sources(res, rows_s, i)

    @pl.when((i >= t_y) & (i < t_b))
    def _():
        j = i - t_y
        d = block_of(j)
        s = 2 * d + jnp.where(j < half, 1, 0)

        @pl.when((j >= 1) & (j <= half))
        def _():
            y_core(block_of(j - 1)).start()

        @pl.when(j > half)
        def _():
            y_chip(block_of(j - 1)).start()

        sel = select_rows(rank_s[s], el)
        gexp = expand_rows(gate_s[s], el)
        o = rows_s[s]
        y = None
        for piece in split3(jnp.transpose(sel * gexp)):
            part = dot(piece, o)
            y = part if y is None else y + part

        @pl.when(j < half)
        def _():
            ysend[d] = y

        @pl.when(j >= half)
        def _():
            y_core(d).wait_recv()
            ytot[d] = y + yrecv[d]

        dys = dot(sel.astype(BF), dyg[s])
        dg = jnp.sum(dys * o.astype(F32), axis=1, keepdims=True)
        spread = sel * dg
        rows = [jnp.sum(spread[e * CAP:(e + 1) * CAP], axis=0, keepdims=True) for e in range(el)]
        rows.append(jnp.zeros((ep - el, tok), F32))
        dgs[s] = jnp.concatenate(rows, axis=0)

    @pl.when(i == t_b)
    def _():
        for k in range(1, ND):
            dg_copy(k).start()

    @pl.when((i >= t_b) & (i < t_x))
    def _():
        n = t_x - 1 - i
        res = []
        for h, do in enumerate(gather_pair(rank_s, dyg, n, gate_s)):
            da = dot_nt(do, w2_ref[h])
            u = us[2 * n + h].astype(F32)
            v = vs[2 * n + h].astype(F32)
            sg = jax.nn.sigmoid(u)
            du = (da * v * sg * (1.0 + u * (1.0 - sg))).astype(BF)
            dv = (da * u * sg).astype(BF)
            du_ref[h] = du
            dv_ref[h] = dv
            res.append(dot_nt(jnp.concatenate([du, dv], axis=1), jnp.concatenate([w1_ref[h], w3_ref[h]], axis=1)))
        to_sources(res, rows_s, n)

    @pl.when(i >= t_x)
    def _():
        j = i - t_x
        d = block_of(j)
        s = 2 * d + jnp.where(j < half, 1, 0)

        @pl.when((j >= 1) & (j <= half))
        def _():
            x_core(block_of(j - 1)).start()

        dx = dot(jnp.transpose(select_rows(rank_s[s], el)).astype(BF), rows_s[s])

        @pl.when(j < half)
        def _():
            xsend[d] = dx

        @pl.when(j >= half)
        def _():
            x_core(d).wait_recv()
            tot = dx + xrecv[d]
            for n, ref in enumerate((x0_ref, x1_ref, x2_ref, x3_ref)):
                @pl.when(d == n)
                def _():
                    ref[...] = tot

    @pl.when(i == last)
    def _():
        for d in range(1, half):
            y_chip(d).wait_recv()
        y_ref[...] = (ytot[0] + ychip[1] + ychip[2] + ychip[3]).astype(BF)
        for k in range(1, ND):
            dg_copy(k).wait_recv()
        first = lax.broadcasted_iota(jnp.int32, (ep, tok), 0)
        live = first < el
        for j in range(top):
            got = jnp.zeros((ep, tok), F32)
            for k in range(ND):
                part = dgs[0] if k == 0 else dgr[k]
                got = got + jnp.where((ids_ref[j:j + 1, :] == first + (p ^ k) * el) & live, part, 0.0)
            dg_ref[j:j + 1, :] = jnp.sum(got, axis=0, keepdims=True)
        for b in range(2):
            for k in range(1, ND):
                tok_copy(b, k).wait_send()
        for d in range(half):
            y_core(d).wait_send()
            x_core(d).wait_send()
            if d:
                y_chip(d).wait_send()
        for k in range(1, ND):
            dg_copy(k).wait_send()
        for n in range(4):
            out_copy(n).wait()


def grad_kernel(rank_ref, gate_ref, x_ref, dy_ref, u_ref, v_ref, du_ref, dv_ref, gw1_ref, gw3_ref, gw2_ref):
    i = pl.program_id(0)
    dos = gather_pair(rank_ref, dy_ref, i, gate_ref)
    for h, xs in enumerate(gather_pair(rank_ref, x_ref, i)):
        gw1_ref[h] = dot_tn(xs, du_ref[h])
        gw3_ref[h] = dot_tn(xs, dv_ref[h])
        u = u_ref[h].astype(F32)
        a = (u * jax.nn.sigmoid(u) * v_ref[h].astype(F32)).astype(BF)
        gw2_ref[h] = dot_tn(a, dos[h])


def solution(mesh):
    grp = ('row', 'col')
    tspec = P(('dp', 'row', 'col'), None)
    wspec = P(grp, None, None)
    gspec = P(('dp', 'row', 'col'), None, None)
    ncol = mesh.shape['col']

    def permute(a, k):
        return lax.ppermute(a, grp, [(p, p ^ k) for p in range(ND)])

    def body(x, ridx, gates, w1, w3, w2, dy):
        tok, d = x.shape
        top = ridx.shape[1]
        el, _, ff = w1.shape
        ep = -(-el // 8) * 8
        m = ND * CAP
        rows = el * CAP
        steps = el // 2
        half = ND // 2
        t_b, t_x = steps + ND, 2 * steps + ND
        sd = jax.ShapeDtypeStruct
        dma = pltpu.SemaphoreType.DMA

        def once(shape):
            return pl.BlockSpec(shape, lambda *_: (0,) * len(shape), pipeline_mode=pl.Buffered(1))

        def pair(shape, index):
            return pl.BlockSpec((2,) + shape, lambda i: (index(i),) + (0,) * len(shape))

        def weight_at(i):
            return jnp.where(i < t_b, jnp.minimum(i, steps - 1), jnp.maximum(t_x - 1 - i, 0))

        def up_at(i):
            return jnp.minimum(i, steps - 1)

        def back_at(i):
            return jnp.clip(t_x - 1 - i, 0, steps - 1)

        prod = 2.0 * el * m * d * ff
        wb = el * d * ff * 2
        hid = sd((el, m, ff), BF)
        anyspec = pl.BlockSpec(memory_space=pl.ANY)
        toks = sd((ND, tok, d), BF)
        tabs = sd((ND, ep, tok), F32)
        block = sd((tok, d), F32)
        vm = pltpu.VMEM
        u, v, du, dv, x0, x1, x2, x3, y, dgates, xg, dyg, rank, gate = pl.pallas_call(
            functools.partial(layer_kernel, el=el, ncol=ncol),
            grid=(t_x + ND,),
            in_specs=[once((top, tok))] * 2 + [once((tok, d))] * 2
            + [pair((d, ff), weight_at)] * 2 + [pair((ff, d), weight_at)],
            out_specs=[pair((m, ff), up_at)] * 2 + [pair((m, ff), back_at)] * 2 + [once((tok, d))] * 5
            + [once((top, tok))] + [anyspec] * 4,
            out_shape=[hid] * 4 + [block] * 4 + [sd((tok, d), BF), sd((top, tok), F32), toks, toks, tabs, tabs],
            scratch_shapes=[vm((ND, tok, d), BF), vm((ND, tok, d), BF), vm((ND, ep, tok), F32),
                            vm((ND, ep, tok), F32), vm((ND, top, tok), jnp.int32), vm((ND, top, tok), F32),
                            vm((el, m, ff), BF), vm((el, m, ff), BF), vm((ND, rows, d), BF)]
            + [vm((half, tok, d), F32)] * 6 + [vm((ND, ep, tok), F32)] * 2
            + [dma((2, ND)), dma((2, ND)), dma((2, 2, ND)), dma((2, half)), dma((2, half)), dma((2, half)),
               dma((2, ND)), dma((4,))],
            compiler_params=pltpu.CompilerParams(dimension_semantics=("arbitrary",), collective_id=0,
                                                 has_side_effects=True, vmem_limit_bytes=VMEM_LIMIT),
            cost_estimate=cost(6 * prod, 6 * wb), name='layer')(ridx.T, gates.T, x, dy, w1, w3, w2)
        dx = x0
        for k, part in enumerate((x1, x2, x3)):
            dx = dx + permute(part, 2 * k + 2)
        dx = dx.astype(BF)

        tab = once((ND, ep, tok))
        src = once((ND, tok, d))
        gw1, gw3, gw2 = pl.pallas_call(
            grad_kernel, grid=(steps,),
            in_specs=[tab] * 2 + [src] * 2 + [pair((m, ff), lambda i: i)] * 4,
            out_specs=[pair((d, ff), lambda i: i)] * 2 + [pair((ff, d), lambda i: i)],
            out_shape=[sd((el, d, ff), F32)] * 2 + [sd((el, ff, d), F32)],
            compiler_params=params(), cost_estimate=cost(3 * prod, 6 * wb), name='grad')(
                rank, gate, xg, dyg, u, v, du, dv)
        return y, dx, dgates.T, gw1, gw3, gw2

    return jax.shard_map(body, mesh=mesh, in_specs=(tspec, tspec, tspec, wspec, wspec, wspec, tspec),
                         out_specs=(tspec, tspec, tspec, gspec, gspec, gspec), check_vma=False)
```

```python
import functools

import jax
import jax.numpy as jnp
from jax import lax
from jax.experimental import pallas as pl
from jax.experimental.pallas import tpu as pltpu
from jax.sharding import PartitionSpec as P


ND = 8
CAP = 24
BF = jnp.bfloat16
F32 = jnp.float32
VMEM_LIMIT = 62 * 1024 * 1024
SLOTS = 3
MESH = pl.DeviceIdType.MESH


def dot(a, b):
    return jnp.dot(a, b, preferred_element_type=F32)


def dot_nt(a, b):
    return lax.dot_general(a, b, (((1,), (1,)), ((), ())), preferred_element_type=F32)


def dot_tn(a, b):
    return lax.dot_general(a, b, (((0,), (0,)), ((), ())), preferred_element_type=F32)


def params(n=1):
    return pltpu.CompilerParams(dimension_semantics=("arbitrary",) * n, vmem_limit_bytes=VMEM_LIMIT)


def cost(flops, nbytes):
    return pl.CostEstimate(flops=int(flops), bytes_accessed=int(nbytes), transcendentals=0)


def select_rows(rank, el):
    r = lax.broadcasted_iota(jnp.int32, (CAP, rank.shape[1]), 0).astype(F32)
    return jnp.concatenate([jnp.where(rank[e:e + 1, :] == r, 1.0, 0.0) for e in range(el)], axis=0)


def expand_rows(mat, el):
    return jnp.concatenate([jnp.broadcast_to(mat[e:e + 1, :], (CAP, mat.shape[1])) for e in range(el)], axis=0)


def split3(g):
    hi = g.astype(BF)
    rest = g - hi.astype(F32)
    mid = rest.astype(BF)
    low = (rest - mid.astype(F32)).astype(BF)
    return hi, mid, low


def peer(k, ncol):
    p = lax.axis_index('row') * ncol + lax.axis_index('col')
    q = p ^ k
    return {'row': q // ncol, 'col': q % ncol}


def gather_pair(rank_ref, src_ref, i, gate_ref=None):
    parts = []
    for s in range(ND):
        rank = rank_ref[s, pl.ds(2 * i, 2), :]
        sel = select_rows(rank, 2)
        rows = dot(sel.astype(BF), src_ref[s])
        if gate_ref is not None:
            gate = expand_rows(gate_ref[s, pl.ds(2 * i, 2), :], 2)
            rows = rows * jnp.sum(sel * gate, axis=1, keepdims=True)
        parts.append(rows)
    return [jnp.concatenate([r[h * CAP:(h + 1) * CAP] for r in parts], axis=0).astype(BF) for h in range(2)]


def to_sources(rows, out_ref, i):
    for s in range(ND):
        part = jnp.concatenate([r[s * CAP:(s + 1) * CAP] for r in rows], axis=0)
        out_ref[s, pl.ds(pl.multiple_of(i * 2 * CAP, 16), 2 * CAP), :] = part.astype(BF)


def block_of(j):
    return (j + 1) % (ND // 2)


def layer_kernel(ids_ref, gates_ref, x_ref, dy_ref, w1_ref, w3_ref, w2_ref,
                 u_out, v_out, du_out, dv_out, x0_ref, x1_ref, x2_ref, x3_ref, y_ref, dg_ref,
                 xg_out, dyg_out, rank_out, gate_out,
                 xg, dyg, rank_s, gate_s, ids_s, gates_s, us, vs, rows_s, ysend, yrecv, ytot, ychip, xrecv,
                 dgs, dgr, w1_s, w3_s, w2_s,
                 ids_sem, gates_sem, tok_sem, yd_sem, yc_sem, xd_sem, dg_sem, out_sem, w_sem, *, el, ncol):
    steps = el // 2
    half = ND // 2
    xsend = ysend
    top, tok = ids_ref.shape
    ep = rank_s.shape[1]
    p = lax.axis_index('row') * ncol + lax.axis_index('col')

    def remote(src, dst, sem, n, k):
        return pltpu.make_async_remote_copy(src_ref=src, dst_ref=dst, send_sem=sem.at[(0,) + n],
                                            recv_sem=sem.at[(1,) + n], device_id=peer(k, ncol), device_id_type=MESH)

    def ids_copy(k):
        return remote(ids_ref, ids_s.at[k], ids_sem, (k,), k)

    def gates_copy(k):
        return remote(gates_ref, gates_s.at[k], gates_sem, (k,), k)

    def tok_copy(b, k):
        buf = (xg, dyg)[b]
        if k in (3, 5, 7):
            return remote(buf.at[k - 1], buf.at[k], tok_sem, (b, k), 1)
        return remote((x_ref, dy_ref)[b], buf.at[k], tok_sem, (b, k), k)

    def y_core(d):
        return remote(ysend.at[d], yrecv.at[d], yd_sem, (d,), 1)

    def y_chip(d):
        return remote(ytot.at[d], ychip.at[d], yc_sem, (d,), 2 * d)

    def x_core(d):
        return remote(xsend.at[d], xrecv.at[d], xd_sem, (d,), 1)

    def dg_copy(k):
        return remote(dgs.at[k], dgr.at[k], dg_sem, (k,), k)

    outs = ((xg, xg_out), (dyg, dyg_out), (rank_s, rank_out), (gate_s, gate_out), (us, u_out), (vs, v_out),
            (us, du_out), (vs, dv_out))

    def out_copy(n):
        return pltpu.make_async_copy(outs[n][0], outs[n][1], out_sem.at[n])

    def weight_copies(t):
        slot = lax.rem(t, SLOTS)
        return [pltpu.make_async_copy(w.at[pl.ds(2 * t, 2)], b.at[slot], w_sem.at[n, slot])
                for n, (w, b) in enumerate(((w1_ref, w1_s), (w3_ref, w3_s), (w2_ref, w2_s)))]

    def fetch(t):
        for c in weight_copies(t):
            c.start()

    def fetched(t):
        for c in weight_copies(t):
            c.wait()

    for t in range(SLOTS):
        fetch(jnp.int32(t))
    barrier = pltpu.get_barrier_semaphore()
    for k in range(1, ND):
        pl.semaphore_signal(barrier, inc=1, device_id=peer(k, ncol), device_id_type=MESH)
    pl.semaphore_wait(barrier, ND - 1)
    for k in range(1, ND):
        ids_copy(k).start()
        gates_copy(k).start()
    xg[0] = x_ref[...]
    dyg[0] = dy_ref[...]
    for k in range(1, ND):
        ids_copy(k).wait()
        gates_copy(k).wait()
    for k in (6, 2, 4, 1):
        tok_copy(0, k).start()
    first = lax.broadcasted_iota(jnp.int32, (ep, tok), 0)
    eid = first + p * el
    live = first < el
    before = lax.broadcasted_iota(jnp.int32, (tok, tok), 0) < lax.broadcasted_iota(jnp.int32, (tok, tok), 1)
    before = jnp.where(before, 1.0, 0.0).astype(BF)
    for s in range(ND):
        ids = ids_ref[...] if s == 0 else ids_s[s]
        gat = gates_ref[...] if s == 0 else gates_s[s]
        hit = jnp.zeros((ep, tok), F32)
        gate = jnp.zeros((ep, tok), F32)
        for j in range(top):
            same = (ids[j:j + 1, :] == eid) & live
            hit = hit + jnp.where(same, 1.0, 0.0)
            gate = gate + jnp.where(same, gat[j:j + 1, :], 0.0)
        rank = dot(hit.astype(BF), before)
        rank_s[s] = jnp.where(hit > 0.0, rank, -1.0)
        gate_s[s] = gate
    for k in (2, 4, 6):
        tok_copy(0, k).wait_recv()
        tok_copy(0, k + 1).start()
    for k in (6, 2, 4, 1):
        tok_copy(1, k).start()
    for k in (1, 3, 5, 7):
        tok_copy(0, k).wait_recv()

    @pl.loop(0, steps)
    def _(i):
        @pl.when(i == steps - 3)
        def _():
            for k in (2, 4, 6):
                tok_copy(1, k).wait_recv()
                tok_copy(1, k + 1).start()

        fetched(i)
        slot = lax.rem(i, SLOTS)
        res = []
        for h, xs in enumerate(gather_pair(rank_s, xg, i)):
            uv = dot(xs, jnp.concatenate([w1_s[slot, h], w3_s[slot, h]], axis=1)).astype(BF)
            ff = uv.shape[1] // 2
            u, v = uv[:, :ff], uv[:, ff:]
            us[2 * i + h] = u
            vs[2 * i + h] = v
            uf = u.astype(F32)
            a = (uf * jax.nn.sigmoid(uf) * v.astype(F32)).astype(BF)
            res.append(dot(a, w2_s[slot, h]))
        to_sources(res, rows_s, i)

        @pl.when(i + SLOTS < steps)
        def _():
            fetch(i + SLOTS)

    for k in (1, 3, 5, 7):
        tok_copy(1, k).wait_recv()
    for n in range(6):
        out_copy(n).start()

    @pl.loop(0, ND)
    def _(j):
        d = block_of(j)
        s = 2 * d + jnp.where(j < half, 1, 0)

        @pl.when((j >= 1) & (j <= half))
        def _():
            y_core(block_of(j - 1)).start()

        @pl.when(j > half)
        def _():
            y_chip(block_of(j - 1)).start()

        sel = select_rows(rank_s[s], el)
        gexp = expand_rows(gate_s[s], el)
        o = rows_s[s]
        y = None
        for piece in split3(jnp.transpose(sel * gexp)):
            part = dot(piece, o)
            y = part if y is None else y + part

        @pl.when(j < half)
        def _():
            ysend[d] = y

        @pl.when(j >= half)
        def _():
            y_core(d).wait_recv()
            ytot[d] = y + yrecv[d]

        dys = dot(sel.astype(BF), dyg[s])
        dg = jnp.sum(dys * o.astype(F32), axis=1, keepdims=True)
        spread = sel * dg
        rows = [jnp.sum(spread[e * CAP:(e + 1) * CAP], axis=0, keepdims=True) for e in range(el)]
        rows.append(jnp.zeros((ep - el, tok), F32))
        dgs[s] = jnp.concatenate(rows, axis=0)

    for k in range(1, ND):
        dg_copy(k).start()
    for d in range(half):
        y_core(d).wait_send()
    for n in (4, 5):
        out_copy(n).wait()

    @pl.loop(0, steps)
    def _(i):
        n = steps - 1 - i

        @pl.when(i >= SLOTS)
        def _():
            fetched(n)

        slot = lax.rem(n, SLOTS)
        res = []
        for h, do in enumerate(gather_pair(rank_s, dyg, n, gate_s)):
            da = dot_nt(do, w2_s[slot, h])
            u = us[2 * n + h].astype(F32)
            v = vs[2 * n + h].astype(F32)
            sg = jax.nn.sigmoid(u)
            du = (da * v * sg * (1.0 + u * (1.0 - sg))).astype(BF)
            dv = (da * u * sg).astype(BF)
            us[2 * n + h] = du
            vs[2 * n + h] = dv
            res.append(dot_nt(jnp.concatenate([du, dv], axis=1), jnp.concatenate([w1_s[slot, h], w3_s[slot, h]], axis=1)))
        to_sources(res, rows_s, n)

        @pl.when(n >= SLOTS)
        def _():
            fetch(n - SLOTS)

    for n in (6, 7):
        out_copy(n).start()

    @pl.loop(0, ND)
    def _(j):
        d = block_of(j)
        s = 2 * d + jnp.where(j < half, 1, 0)

        @pl.when((j >= 1) & (j <= half))
        def _():
            x_core(block_of(j - 1)).start()

        dx = dot(jnp.transpose(select_rows(rank_s[s], el)).astype(BF), rows_s[s])

        @pl.when(j < half)
        def _():
            xsend[d] = dx

        @pl.when(j >= half)
        def _():
            x_core(d).wait_recv()
            tot = dx + xrecv[d]
            for n, ref in enumerate((x0_ref, x1_ref, x2_ref, x3_ref)):
                @pl.when(d == n)
                def _():
                    ref[...] = tot

    for d in range(1, half):
        y_chip(d).wait_recv()
    y_ref[...] = (ytot[0] + ychip[1] + ychip[2] + ychip[3]).astype(BF)
    for k in range(1, ND):
        dg_copy(k).wait_recv()
    first = lax.broadcasted_iota(jnp.int32, (ep, tok), 0)
    live = first < el
    for j in range(top):
        got = jnp.zeros((ep, tok), F32)
        for k in range(ND):
            part = dgs[0] if k == 0 else dgr[k]
            got = got + jnp.where((ids_ref[j:j + 1, :] == first + (p ^ k) * el) & live, part, 0.0)
        dg_ref[j:j + 1, :] = jnp.sum(got, axis=0, keepdims=True)
    for b in range(2):
        for k in range(1, ND):
            tok_copy(b, k).wait_send()
    for d in range(half):
        x_core(d).wait_send()
        if d:
            y_chip(d).wait_send()
    for k in range(1, ND):
        dg_copy(k).wait_send()
    for n in (0, 1, 2, 3, 6, 7):
        out_copy(n).wait()


def grad_kernel(rank_ref, gate_ref, x_ref, dy_ref, u_ref, v_ref, du_ref, dv_ref, gw1_ref, gw3_ref, gw2_ref):
    i = pl.program_id(0)
    dos = gather_pair(rank_ref, dy_ref, i, gate_ref)
    for h, xs in enumerate(gather_pair(rank_ref, x_ref, i)):
        gw1_ref[h] = dot_tn(xs, du_ref[h])
        gw3_ref[h] = dot_tn(xs, dv_ref[h])
        u = u_ref[h].astype(F32)
        a = (u * jax.nn.sigmoid(u) * v_ref[h].astype(F32)).astype(BF)
        gw2_ref[h] = dot_tn(a, dos[h])


def solution(mesh):
    grp = ('row', 'col')
    tspec = P(('dp', 'row', 'col'), None)
    wspec = P(grp, None, None)
    gspec = P(('dp', 'row', 'col'), None, None)
    ncol = mesh.shape['col']

    def permute(a, k):
        return lax.ppermute(a, grp, [(p, p ^ k) for p in range(ND)])

    def body(x, ridx, gates, w1, w3, w2, dy):
        tok, d = x.shape
        top = ridx.shape[1]
        el, _, ff = w1.shape
        ep = -(-el // 8) * 8
        m = ND * CAP
        rows = el * CAP
        steps = el // 2
        half = ND // 2
        sd = jax.ShapeDtypeStruct
        dma = pltpu.SemaphoreType.DMA

        def once(shape):
            return pl.BlockSpec(shape, lambda *_: (0,) * len(shape), pipeline_mode=pl.Buffered(1))

        def pair(shape, index):
            return pl.BlockSpec((2,) + shape, lambda i: (index(i),) + (0,) * len(shape))

        prod = 2.0 * el * m * d * ff
        wb = el * d * ff * 2
        hid = sd((el, m, ff), BF)
        anyspec = pl.BlockSpec(memory_space=pl.ANY)
        toks = sd((ND, tok, d), BF)
        tabs = sd((ND, ep, tok), F32)
        block = sd((tok, d), F32)
        vm = pltpu.VMEM
        vmem = pl.BlockSpec(memory_space=pltpu.VMEM)
        u, v, du, dv, x0, x1, x2, x3, y, dgates, xg, dyg, rank, gate = pl.pallas_call(
            functools.partial(layer_kernel, el=el, ncol=ncol),
            in_specs=[vmem] * 4 + [anyspec] * 3,
            out_specs=[anyspec] * 4 + [vmem] * 6 + [anyspec] * 4,
            out_shape=[hid] * 4 + [block] * 4 + [sd((tok, d), BF), sd((top, tok), F32), toks, toks, tabs, tabs],
            scratch_shapes=[vm((ND, tok, d), BF), vm((ND, tok, d), BF), vm((ND, ep, tok), F32),
                            vm((ND, ep, tok), F32), vm((ND, top, tok), jnp.int32), vm((ND, top, tok), F32),
                            vm((el, m, ff), BF), vm((el, m, ff), BF), vm((ND, rows, d), BF)]
            + [vm((half, tok, d), F32)] * 5 + [vm((ND, ep, tok), F32)] * 2
            + [vm((SLOTS, 2, d, ff), BF)] * 2 + [vm((SLOTS, 2, ff, d), BF)]
            + [dma((2, ND)), dma((2, ND)), dma((2, 2, ND)), dma((2, half)), dma((2, half)), dma((2, half)),
               dma((2, ND)), dma((8,)), dma((3, SLOTS))],
            compiler_params=pltpu.CompilerParams(collective_id=0, has_side_effects=True, vmem_limit_bytes=VMEM_LIMIT),
            cost_estimate=cost(6 * prod, 6 * wb), name='layer')(ridx.T, gates.T, x, dy, w1, w3, w2)
        dx = x0
        for k, part in enumerate((x1, x2, x3)):
            dx = dx + permute(part, 2 * k + 2)
        dx = dx.astype(BF)

        tab = once((ND, ep, tok))
        src = once((ND, tok, d))
        gw1, gw3, gw2 = pl.pallas_call(
            grad_kernel, grid=(steps,),
            in_specs=[tab] * 2 + [src] * 2 + [pair((m, ff), lambda i: i)] * 4,
            out_specs=[pair((d, ff), lambda i: i)] * 2 + [pair((ff, d), lambda i: i)],
            out_shape=[sd((el, d, ff), F32)] * 2 + [sd((el, ff, d), F32)],
            compiler_params=params(), cost_estimate=cost(3 * prod, 6 * wb), name='grad')(
                rank, gate, xg, dyg, u, v, du, dv)
        return y, dx, dgates.T, gw1, gw3, gw2

    return jax.shard_map(body, mesh=mesh, in_specs=(tspec, tspec, tspec, wspec, wspec, wspec, tspec),
                         out_specs=(tspec, tspec, tspec, gspec, gspec, gspec), check_vma=False)
```
